32 devices in a mesh: section: 4 (over x, core), expert: 8 (over z, y).
Axes of the slice: x: 2, y: 2, z: 4, core: 2. Of those that a mesh axis runs over, the one named last changes fastest.
Arguments:
- x_fwd: bfloat16 [4, 1024, 3584], P('section', 'expert'), may hold values from -6 to 6
- routes_fwd: int32 [4, 1024, 2], P('section', 'expert'), may hold values from 0 to 3, all different within a row; in each aligned block of 128 rows (0 to 127, 128 to 255, ..., all dimensions but the last counted through in order) at most 96 rows name the same one
- affinity_fwd: float32 [4, 1024, 2], P('section', 'expert'), may hold values from 0.1 to 1
- x_bwd: bfloat16 [4, 1024, 3584], P('section', 'expert'), may hold values from -6 to 6
- grad_bwd: bfloat16 [4, 1024, 3584], P('section', 'expert'), may hold values from -6 to 6
- routes_bwd: int32 [4, 1024, 2], P('section', 'expert'), may hold values from 0 to 3, all different within a row; in each aligned block of 128 rows (0 to 127, 128 to 255, ..., all dimensions but the last counted through in order) at most 96 rows name the same one
- affinity_bwd: float32 [4, 1024, 2], P('section', 'expert'), may hold values from 0.1 to 1
- up_weight: bfloat16 [4, 3584, 4096], P('section', None, 'expert'), may hold values from -0.09375 to 0.09375
- down_weight: bfloat16 [4, 4096, 3584], P('section', 'expert'), may hold values from -0.1875 to 0.1875
Outputs:
- fwd_next: bfloat16 [4, 1024, 3584], P('section', 'expert')
- bwd_next: bfloat16 [4, 1024, 3584], P('section', 'expert')
The draws below stay inside these ranges and needn't reach their ends.
Inputs may be any that keep to these rules, and one draw needn't show every extreme that they name: `routes_fwd`: each row names 2 different experts; in each section, among the 128 rows of one device (aligned blocks), no expert is named more than 96 times, a bound that some block reaches. `routes_bwd`: each row names 2 different experts; in each section, among the 128 rows of one device (aligned blocks), no expert is named more than 96 times, a bound that some block reaches.
All inputs are finite; a program needn't handle non-finite values.
Results may differ from the reference program's by a relative error of at most 0.0041.
Values may be sent and summed in bfloat16 or wider, within the bound.
A program may use at most 128 MiB of HBM per device.

```python
import math
import jax
import jax.numpy as jnp
import numpy as np
from jax import lax

D = 3584
HID = 1024
TOP = 2
TOK_DEV = 128
SECTIONS = 4
EXPERTS = 4
TOKENS = 1024
CAP = 96
N_EXPERT = 8


def steps_of(key, shape, split, least, high):
    level, own = 1.0, jax.random.fold_in(key, 6)
    for position, shards_of in split:
        steps = jnp.exp(jax.random.uniform(jax.random.fold_in(own, position), (shards_of,), jnp.float32, least / len(split), high / len(split)))
        level = level * jnp.repeat(steps, shape[position] // shards_of).reshape([-1 if axis == position else 1 for axis in range(len(shape))])
    return level


def assign_block(stream_key, own, number, rows, count, top, limit, lean):
    sequence = jax.random.permutation(stream_key, count)
    crowded, ordinary = portions_of(count, rows * top, limit, lean, True), portions_of(count, rows * top, limit, lean, False)
    places = jnp.arange(count)

    def named(tallies, rotation):
        used = int((tallies > 0).sum())
        fixed = max(1, used // 4)
        passed = fixed + (places - fixed + rotation * (used - fixed)) % max(1, count - fixed)
        return jnp.zeros((count,), jnp.int32).at[sequence[jnp.where(places < fixed, places, passed)]].set(jnp.asarray(tallies, jnp.int32))

    tallies = jnp.where(number % 4 == 0, named(crowded, number // 4), named(ordinary, number - number // 4 - 1))
    mixed = jax.random.permutation(jax.random.fold_in(own, 3), count)
    giver, sink = mixed[0:count // 2 * 2:2], mixed[1:count // 2 * 2:2]
    slack = jnp.minimum(tallies[giver] - 1, limit - tallies[sink]) // 2
    slack = jnp.where((giver == sequence[0]) | (sink == sequence[0]) | (tallies[sink] == 0), 0, jnp.maximum(slack, 0))
    passed = jax.random.randint(jax.random.fold_in(own, 4), (count // 2,), 0, 1 << 20) % (slack + 1)
    tallies = tallies.at[giver].add(-passed).at[sink].add(passed)
    labels = jnp.searchsorted(jnp.cumsum(tallies), jnp.arange(rows * top), side="right").astype(jnp.int32)
    listing = labels.reshape(top, rows).T
    listing = listing[jax.random.permutation(jax.random.fold_in(own, 1), rows)]
    rotation = jax.random.randint(jax.random.fold_in(own, 2), (rows, 1), 0, top)
    return jnp.take_along_axis(listing, (jnp.arange(top)[None, :] + rotation) % top, axis=1)


def portions_of(count, total, limit, skew, full):
    portions = [(1 << 20) // math.isqrt(standing ** skew) + 1 for standing in range(1, count + 1)]
    largest = limit if full else min(limit, max(-(-total // count), total * portions[0] // sum(portions)))
    least = 1 if total - largest >= count - 1 else 0
    holding, surplus = [largest] + [least] * (count - 1), total - largest - least * (count - 1)
    while surplus > 0:
        free = [i for i in range(1, count) if holding[i] < largest] or [i for i in range(1, count) if holding[i] < limit]
        whole, left = sum([portions[i] for i in free]), surplus
        for i in free:
            extra = min(limit - holding[i], max(1, left * portions[i] // whole), surplus)
            holding[i] = holding[i] + extra
            surplus = surplus - extra
    return np.array(holding)


def gaussian(key, dims, deviation, bound, split=(), kind=jnp.bfloat16):
    array = deviation * jax.random.normal(key, dims, jnp.float32)
    if split:
        array = array * steps_of(key, dims, split, -0.22, 0.18)
    return jnp.clip(array, -bound, bound).astype(kind)


def setup_inputs(seed: int = 0) -> dict:
    keys = jax.random.split(jax.random.key(seed), 10)
    x_fwd = gaussian(keys[0], (SECTIONS, TOKENS, D), 1.0, 6.0, ((0, 4), (1, 8)))
    routes_fwd_keys = jax.random.split(jax.random.fold_in(keys[1], 1), SECTIONS * TOKENS // TOK_DEV)
    routes_fwd_turns = jax.random.permutation(jax.random.fold_in(keys[1], 3), SECTIONS * TOKENS // TOK_DEV)
    routes_fwd = jax.vmap(lambda own, number: assign_block(jax.random.fold_in(keys[1], 2), own, number, TOK_DEV, EXPERTS, TOP, CAP, 2))(routes_fwd_keys, routes_fwd_turns).reshape((SECTIONS, TOKENS, TOP))
    affinity_fwd = jnp.clip(jnp.exp(math.log(1.0) - 2.3025851 * jax.random.uniform(keys[2], (SECTIONS, TOKENS, TOP), jnp.float32) ** steps_of(keys[2], (SECTIONS, TOKENS, TOP), ((0, 4), (1, 8)), -0.2, 0.2)), 0.1, 1.0)
    x_bwd = gaussian(keys[3], (SECTIONS, TOKENS, D), 1.0, 6.0, ((0, 4), (1, 8)))
    grad_bwd = gaussian(keys[4], (SECTIONS, TOKENS, D), 1.0, 6.0, ((0, 4), (1, 8)))
    routes_bwd_keys = jax.random.split(jax.random.fold_in(keys[5], 1), SECTIONS * TOKENS // TOK_DEV)
    routes_bwd_turns = jax.random.permutation(jax.random.fold_in(keys[5], 3), SECTIONS * TOKENS // TOK_DEV)
    routes_bwd = jax.vmap(lambda own, number: assign_block(jax.random.fold_in(keys[5], 2), own, number, TOK_DEV, EXPERTS, TOP, CAP, 2))(routes_bwd_keys, routes_bwd_turns).reshape((SECTIONS, TOKENS, TOP))
    affinity_bwd = jnp.clip(jnp.exp(math.log(1.0) - 2.3025851 * jax.random.uniform(keys[6], (SECTIONS, TOKENS, TOP), jnp.float32) ** steps_of(keys[6], (SECTIONS, TOKENS, TOP), ((0, 4), (1, 8)), -0.2, 0.2)), 0.1, 1.0)
    up_weight = gaussian(keys[7], (SECTIONS, D, EXPERTS * HID), D ** -0.5, 0.09375, ((0, 4), (2, 8)))
    down_weight = gaussian(keys[8], (SECTIONS, EXPERTS * HID, D), HID ** -0.5, 0.1875, ((0, 4), (1, 8)))
    return {"x_fwd": x_fwd, "routes_fwd": routes_fwd, "affinity_fwd": affinity_fwd, "x_bwd": x_bwd, "grad_bwd": grad_bwd, "routes_bwd": routes_bwd, "affinity_bwd": affinity_bwd, "up_weight": up_weight, "down_weight": down_weight}


def silu_grad(values):
    sigma = jax.nn.sigmoid(values)
    return sigma * (1.0 + values * (1.0 - sigma))

def expert_pass(rows_fwd, rows_saved, rows_grad, up_block, down_block):
    half_count = HID // 2
    sums_fwd = jnp.zeros((rows_fwd.shape[0], D), jnp.float32)
    sums_bwd = jnp.zeros((rows_fwd.shape[0], D), jnp.float32)
    for half_id in range(2):
        up_part = up_block[:, half_id * half_count:(half_id + 1) * half_count]
        down_part = down_block[half_id * half_count:(half_id + 1) * half_count, :]
        hidden = jax.nn.silu(jnp.dot(rows_fwd, up_part, preferred_element_type=jnp.float32)).astype(jnp.bfloat16)
        part_fwd = jnp.dot(hidden, down_part, preferred_element_type=jnp.float32).astype(jnp.bfloat16)
        pre_act = jnp.dot(rows_saved, up_part, preferred_element_type=jnp.float32)
        hidden_grad = jnp.dot(rows_grad, down_part.T, preferred_element_type=jnp.float32)
        pre_grad = (hidden_grad * silu_grad(pre_act)).astype(jnp.bfloat16)
        part_bwd = jnp.dot(pre_grad, up_part.T, preferred_element_type=jnp.float32).astype(jnp.bfloat16)
        sums_fwd = sums_fwd + part_fwd.astype(jnp.float32)
        sums_bwd = sums_bwd + part_bwd.astype(jnp.float32)
    return (sums_fwd.astype(jnp.bfloat16), sums_bwd.astype(jnp.bfloat16))

def combine(inputs, results, affinity):
    weights = affinity / lax.optimization_barrier(jnp.sum(affinity, -1, keepdims=True))
    routed = results.reshape(TOKENS, TOP, D).astype(jnp.float32)
    return (inputs.astype(jnp.float32) + lax.optimization_barrier(jnp.sum(weights[..., None] * routed, 1))).astype(jnp.bfloat16)

def reference(x_fwd, routes_fwd, affinity_fwd, x_bwd, grad_bwd, routes_bwd, affinity_bwd, up_weight, down_weight):
    total = TOKENS * TOP
    rows = N_EXPERT * CAP
    zero_row = jnp.zeros((1, D), jnp.bfloat16)
    layer_outs = []
    input_grads = []
    for section_id in range(SECTIONS):
        inputs_fwd = jnp.concatenate([x_fwd[section_id], zero_row], 0)
        inputs_saved = jnp.concatenate([x_bwd[section_id], zero_row], 0)
        inputs_grad = jnp.concatenate([grad_bwd[section_id], zero_row], 0)
        flat_fwd = routes_fwd[section_id].reshape(-1)
        flat_bwd = routes_bwd[section_id].reshape(-1)
        up_section = up_weight[section_id]
        down_section = down_weight[section_id]

        def one_expert(carry, expert_id):
            results_fwd, results_bwd = carry
            index_fwd = jnp.nonzero(flat_fwd == expert_id, size=rows, fill_value=total)[0].astype(jnp.int32)
            index_bwd = jnp.nonzero(flat_bwd == expert_id, size=rows, fill_value=total)[0].astype(jnp.int32)
            up_block = lax.dynamic_slice_in_dim(up_section, (expert_id * HID).astype(jnp.int32), HID, 1)
            down_block = lax.dynamic_slice_in_dim(down_section, (expert_id * HID).astype(jnp.int32), HID, 0)
            token_fwd = index_fwd // TOP
            token_bwd = index_bwd // TOP
            outs_fwd, outs_bwd = expert_pass(inputs_fwd[token_fwd], inputs_saved[token_bwd], inputs_grad[token_bwd], up_block, down_block)
            results_fwd = results_fwd.at[index_fwd].set(outs_fwd)
            results_bwd = results_bwd.at[index_bwd].set(outs_bwd)
            return ((results_fwd, results_bwd), None)
        start = jnp.zeros((total + 1, D), jnp.bfloat16)
        (results_fwd, results_bwd), _ = lax.scan(one_expert, (start, start), jnp.arange(EXPERTS, dtype=jnp.int32))
        layer_outs.append(combine(x_fwd[section_id], results_fwd[:total], affinity_fwd[section_id]))
        input_grads.append(combine(grad_bwd[section_id], results_bwd[:total], affinity_bwd[section_id]))
    layer_out = jnp.stack(layer_outs)
    input_grad = jnp.stack(input_grads)
    return (jnp.roll(layer_out, 1, 0), jnp.roll(input_grad, -1, 0))
```

```python
import jax
import jax.numpy as jnp
from jax import lax
from jax.sharding import PartitionSpec as P


def from_partner_2(block, axis, apart):
    count = lax.axis_size(axis)
    route = []
    for low in range(count):
        high = low | 1 << apart
        if high != low and high < count:
            route += [(low, high), (high, low)]
    return lax.ppermute(block, axis, route)


def shifted(shard, axis, by):
    size = lax.axis_size(axis)
    return lax.ppermute(shard, axis, [(i, (i + by) % size) for i in range(size)])


def silu_grad(values):
    sigma = jax.nn.sigmoid(values)
    return sigma * (1.0 + values * (1.0 - sigma))


def slot_table(routes, experts, capacity):
    flat_routes = routes.reshape(-1)
    entries = flat_routes.shape[0]
    onehot = (flat_routes[:, None] == jnp.arange(experts, dtype=jnp.int32)[None, :]).astype(
        jnp.int32
    )
    before = jnp.cumsum(onehot, 0) - onehot
    position = jnp.sum(before * onehot, 1)
    slot_of = flat_routes * capacity + position
    source = (
        jnp.full((experts * capacity,), entries, jnp.int32)
        .at[slot_of]
        .set(jnp.arange(entries, dtype=jnp.int32))
    )
    return (slot_of, source)


def serve_rows(received, up_half, down_half):
    sources = received.shape[0]
    slots = received.shape[2]
    model_width = received.shape[3]
    row_count = sources * slots
    rows_fwd = received[:, 0].reshape(row_count, model_width)
    rows_saved = received[:, 1].reshape(row_count, model_width)
    rows_grad = received[:, 2].reshape(row_count, model_width)
    against_rows = (((1,), (1,)), ((), ()))
    hidden = jax.nn.silu(jnp.dot(rows_fwd, up_half, preferred_element_type=jnp.float32)).astype(
        jnp.bfloat16
    )
    part_fwd = jnp.dot(hidden, down_half, preferred_element_type=jnp.float32).astype(jnp.bfloat16)
    pre_act = jnp.dot(rows_saved, up_half, preferred_element_type=jnp.float32)
    hidden_grad = lax.dot_general(
        rows_grad, down_half, against_rows, preferred_element_type=jnp.float32
    )
    pre_grad = (hidden_grad * silu_grad(pre_act)).astype(jnp.bfloat16)
    part_bwd = lax.dot_general(
        pre_grad, up_half, against_rows, preferred_element_type=jnp.float32
    ).astype(jnp.bfloat16)
    return jnp.stack(
        [
            part_fwd.reshape(sources, slots, model_width),
            part_bwd.reshape(sources, slots, model_width),
        ],
        1,
    )


def combine(inputs, routed_rows, affinity):
    tokens = inputs.shape[0]
    top_count = affinity.shape[1]
    weights = affinity / jnp.sum(affinity, -1, keepdims=True)
    routed = routed_rows.reshape(tokens, top_count, inputs.shape[1]).astype(jnp.float32)
    return (inputs.astype(jnp.float32) + jnp.sum(weights[..., None] * routed, 1)).astype(
        jnp.bfloat16
    )


def general_path(
    x_fwd,
    routes_fwd,
    affinity_fwd,
    x_bwd,
    grad_bwd,
    routes_bwd,
    affinity_bwd,
    up_weight,
    down_weight,
):
    devices = lax.axis_size("expert")
    experts = devices // 2
    tokens = x_fwd.shape[1]
    model_width = x_fwd.shape[2]
    top_count = routes_fwd.shape[2]
    capacity = 3 * tokens * top_count // devices
    half_slots = capacity // 2
    up_half = up_weight[0]
    down_half = down_weight[0]
    slot_fwd, source_fwd = slot_table(routes_fwd[0], experts, capacity)
    slot_bwd, source_bwd = slot_table(routes_bwd[0], experts, capacity)
    zero_row = jnp.zeros((1, model_width), jnp.bfloat16)
    row_table = jnp.concatenate([x_fwd[0], zero_row, x_bwd[0], zero_row, grad_bwd[0], zero_row], 0)
    stride = tokens + 1
    token_fwd = (source_fwd // top_count).reshape(experts, capacity)
    token_bwd = (source_bwd // top_count).reshape(experts, capacity)
    gather_index = jnp.stack([token_fwd, token_bwd + stride, token_bwd + 2 * stride], 1)
    send_index = (
        gather_index.reshape(experts, 3, 2, half_slots)
        .transpose(0, 2, 1, 3)
        .reshape(devices, 3, half_slots)
    )
    outgoing = row_table[send_index]
    received = lax.all_to_all(outgoing, "expert", split_axis=0, concat_axis=0, tiled=True)
    partner = from_partner_2(received, "expert", 0)
    result = serve_rows(jnp.concatenate([received, partner], 2), up_half, down_half)
    piece_slots = received.shape[2]
    from_partner = from_partner_2(result[:, :, piece_slots:], "expert", 0)
    summed = (
        result[:, :, :piece_slots].astype(jnp.float32) + from_partner.astype(jnp.float32)
    ).astype(jnp.bfloat16)
    returned = lax.all_to_all(summed, "expert", split_axis=0, concat_axis=0, tiled=True)
    flat_back = returned.reshape(-1, model_width)

    def back_index(slot_of, member):
        expert_id = slot_of // capacity
        within = slot_of % capacity
        return (
            (2 * expert_id + within // half_slots) * 2 + member
        ) * half_slots + within % half_slots

    index_fwd = back_index(slot_fwd, 0)
    index_bwd = back_index(slot_bwd, 1)
    layer_out = combine(x_fwd[0], flat_back[index_fwd], affinity_fwd[0])
    input_grad = combine(grad_bwd[0], flat_back[index_bwd], affinity_bwd[0])
    fwd_next = shifted(layer_out[None], "section", 1)
    bwd_next = shifted(input_grad[None], "section", -1)
    return (fwd_next, bwd_next)


def dense_weights(routes, affinity, experts):
    weights = affinity / jnp.sum(affinity, -1, keepdims=True)
    named = routes[:, :, None] == jnp.arange(experts, dtype=jnp.int32)
    return jnp.sum(jnp.where(named, weights[:, :, None], 0.0), 1)


def line_pairs(experts, low, high, by):
    return [
        (2 * z + half, 2 * (z + by) + half) for z in range(low, high) for half in range(2)
    ]


def gather_line(block, experts, place):
    right, left = [], []
    passed_right, passed_left = block, block
    for step in range(1, experts):
        passed_right = lax.ppermute(
            passed_right, "expert", line_pairs(experts, step - 1, experts - 1, 1)
        )
        passed_left = lax.ppermute(
            passed_left, "expert", line_pairs(experts, 1, experts - step + 1, -1)
        )
        right.append(passed_right)
        left.append(passed_left)
    slots = [block]
    for ahead in range(1, experts):
        from_left_end = right[experts - ahead - 1]
        from_right_end = left[ahead - 1]
        slots.append(jnp.where(place + ahead < experts, from_right_end, from_left_end))
    return jnp.concatenate(slots, 0)


def reduce_line(parts, experts):
    right, left = None, None
    for step in range(1, experts):
        send_right, send_left = parts[experts - step], parts[step]
        if right is not None:
            send_right = send_right + right.astype(jnp.float32)
            send_left = send_left + left.astype(jnp.float32)
        right = lax.ppermute(
            send_right.astype(jnp.bfloat16), "expert", line_pairs(experts, 0, step, 1)
        )
        left = lax.ppermute(
            send_left.astype(jnp.bfloat16),
            "expert",
            line_pairs(experts, experts - step, experts, -1),
        )
    return parts[0] + right.astype(jnp.float32) + left.astype(jnp.float32)


def own_expert_weights(dense, experts, place):
    columns = []
    for ahead in range(experts):
        target = lax.rem(place + experts - ahead, experts)
        column = lax.dynamic_index_in_dim(dense, target, 1, keepdims=False)
        if ahead:
            route = [
                (2 * z + half, 2 * ((z - ahead) % experts) + half)
                for z in range(experts)
                for half in range(2)
            ]
            column = lax.ppermute(column, "expert", route)
        columns.append(column)
    return jnp.concatenate(columns, 0)


AGAINST_ROWS = (((1,), (1,)), ((), ()))


def forward_half(rows, up_half, down_half):
    hidden = jax.nn.silu(jnp.dot(rows, up_half, preferred_element_type=jnp.float32))
    return jnp.dot(
        hidden.astype(jnp.bfloat16), down_half, preferred_element_type=jnp.float32
    ).astype(jnp.bfloat16)


def backward_half(rows_saved, rows_grad, up_half, down_half):
    pre_act = jnp.dot(rows_saved, up_half, preferred_element_type=jnp.float32)
    hidden_grad = lax.dot_general(
        rows_grad, down_half, AGAINST_ROWS, preferred_element_type=jnp.float32
    )
    pre_grad = (hidden_grad * silu_grad(pre_act)).astype(jnp.bfloat16)
    return lax.dot_general(
        pre_grad, up_half, AGAINST_ROWS, preferred_element_type=jnp.float32
    ).astype(jnp.bfloat16)


def weighted_blocks(first, second, weights, experts):
    total = (first.astype(jnp.float32) + second.astype(jnp.float32)) * weights[:, None]
    tokens = total.shape[0] // experts
    return [total[i * tokens : (i + 1) * tokens] for i in range(experts)]


def dense_path(
    x_fwd,
    routes_fwd,
    affinity_fwd,
    x_bwd,
    grad_bwd,
    routes_bwd,
    affinity_bwd,
    up_weight,
    down_weight,
):
    experts = lax.axis_size("expert") // 2
    place = lax.axis_index("expert") // 2
    up_half, down_half = up_weight[0], down_weight[0]
    up_other = from_partner_2(up_half, "expert", 0)
    down_other = from_partner_2(down_half, "expert", 0)
    weights_fwd = own_expert_weights(
        dense_weights(routes_fwd[0], affinity_fwd[0], experts), experts, place
    )
    weights_bwd = own_expert_weights(
        dense_weights(routes_bwd[0], affinity_bwd[0], experts), experts, place
    )
    rows_fwd = gather_line(x_fwd[0], experts, place)
    rows_saved = gather_line(x_bwd[0], experts, place)
    rows_grad = gather_line(grad_bwd[0], experts, place)
    parts_fwd = weighted_blocks(
        forward_half(rows_fwd, up_half, down_half),
        forward_half(rows_fwd, up_other, down_other),
        weights_fwd,
        experts,
    )
    layer_out = (x_fwd[0].astype(jnp.float32) + reduce_line(parts_fwd, experts)).astype(
        jnp.bfloat16
    )
    fwd_next = shifted(layer_out[None], "section", 1)
    parts_bwd = weighted_blocks(
        backward_half(rows_saved, rows_grad, up_half, down_half),
        backward_half(rows_saved, rows_grad, up_other, down_other),
        weights_bwd,
        experts,
    )
    input_grad = (grad_bwd[0].astype(jnp.float32) + reduce_line(parts_bwd, experts)).astype(
        jnp.bfloat16
    )
    bwd_next = shifted(input_grad[None], "section", -1)
    return (fwd_next, bwd_next)


def per_device(*args):
    experts = lax.axis_size("expert") // 2
    top_count = args[1].shape[2]
    if 2 * top_count >= experts:
        return dense_path(*args)
    return general_path(*args)


def solution(mesh):
    in_specs = (
        P("section", "expert", None),
        P("section", "expert", None),
        P("section", "expert", None),
        P("section", "expert", None),
        P("section", "expert", None),
        P("section", "expert", None),
        P("section", "expert", None),
        P("section", None, "expert"),
        P("section", "expert", None),
    )
    out_specs = (P("section", "expert", None), P("section", "expert", None))
    return jax.shard_map(
        per_device, mesh=mesh, in_specs=in_specs, out_specs=out_specs, check_vma=False
    )
```

```python
import jax
import jax.numpy as jnp
from jax import lax
from jax.sharding import PartitionSpec as P


def from_partner_2(block, axis, apart):
    count = lax.axis_size(axis)
    route = []
    for low in range(count):
        high = low | 1 << apart
        if high != low and high < count:
            route += [(low, high), (high, low)]
    return lax.ppermute(block, axis, route)


def shifted(shard, axis, by):
    size = lax.axis_size(axis)
    return lax.ppermute(shard, axis, [(i, (i + by) % size) for i in range(size)])


def silu_grad(values):
    sigma = jax.nn.sigmoid(values)
    return sigma * (1.0 + values * (1.0 - sigma))


def slot_table(routes, experts, capacity):
    flat_routes = routes.reshape(-1)
    entries = flat_routes.shape[0]
    onehot = (flat_routes[:, None] == jnp.arange(experts, dtype=jnp.int32)[None, :]).astype(
        jnp.int32
    )
    before = jnp.cumsum(onehot, 0) - onehot
    position = jnp.sum(before * onehot, 1)
    slot_of = flat_routes * capacity + position
    source = (
        jnp.full((experts * capacity,), entries, jnp.int32)
        .at[slot_of]
        .set(jnp.arange(entries, dtype=jnp.int32))
    )
    return (slot_of, source)


def serve_rows(received, up_half, down_half):
    sources = received.shape[0]
    slots = received.shape[2]
    model_width = received.shape[3]
    row_count = sources * slots
    rows_fwd = received[:, 0].reshape(row_count, model_width)
    rows_saved = received[:, 1].reshape(row_count, model_width)
    rows_grad = received[:, 2].reshape(row_count, model_width)
    against_rows = (((1,), (1,)), ((), ()))
    hidden = jax.nn.silu(jnp.dot(rows_fwd, up_half, preferred_element_type=jnp.float32)).astype(
        jnp.bfloat16
    )
    part_fwd = jnp.dot(hidden, down_half, preferred_element_type=jnp.float32).astype(jnp.bfloat16)
    pre_act = jnp.dot(rows_saved, up_half, preferred_element_type=jnp.float32)
    hidden_grad = lax.dot_general(
        rows_grad, down_half, against_rows, preferred_element_type=jnp.float32
    )
    pre_grad = (hidden_grad * silu_grad(pre_act)).astype(jnp.bfloat16)
    part_bwd = lax.dot_general(
        pre_grad, up_half, against_rows, preferred_element_type=jnp.float32
    ).astype(jnp.bfloat16)
    return jnp.stack(
        [
            part_fwd.reshape(sources, slots, model_width),
            part_bwd.reshape(sources, slots, model_width),
        ],
        1,
    )


def combine(inputs, routed_rows, affinity):
    tokens = inputs.shape[0]
    top_count = affinity.shape[1]
    weights = affinity / jnp.sum(affinity, -1, keepdims=True)
    routed = routed_rows.reshape(tokens, top_count, inputs.shape[1]).astype(jnp.float32)
    return (inputs.astype(jnp.float32) + jnp.sum(weights[..., None] * routed, 1)).astype(
        jnp.bfloat16
    )


def general_path(
    x_fwd,
    routes_fwd,
    affinity_fwd,
    x_bwd,
    grad_bwd,
    routes_bwd,
    affinity_bwd,
    up_weight,
    down_weight,
):
    devices = lax.axis_size("expert")
    experts = devices // 2
    tokens = x_fwd.shape[1]
    model_width = x_fwd.shape[2]
    top_count = routes_fwd.shape[2]
    capacity = 3 * tokens * top_count // devices
    half_slots = capacity // 2
    up_half = up_weight[0]
    down_half = down_weight[0]
    slot_fwd, source_fwd = slot_table(routes_fwd[0], experts, capacity)
    slot_bwd, source_bwd = slot_table(routes_bwd[0], experts, capacity)
    zero_row = jnp.zeros((1, model_width), jnp.bfloat16)
    row_table = jnp.concatenate([x_fwd[0], zero_row, x_bwd[0], zero_row, grad_bwd[0], zero_row], 0)
    stride = tokens + 1
    token_fwd = (source_fwd // top_count).reshape(experts, capacity)
    token_bwd = (source_bwd // top_count).reshape(experts, capacity)
    gather_index = jnp.stack([token_fwd, token_bwd + stride, token_bwd + 2 * stride], 1)
    send_index = (
        gather_index.reshape(experts, 3, 2, half_slots)
        .transpose(0, 2, 1, 3)
        .reshape(devices, 3, half_slots)
    )
    outgoing = row_table[send_index]
    received = lax.all_to_all(outgoing, "expert", split_axis=0, concat_axis=0, tiled=True)
    partner = from_partner_2(received, "expert", 0)
    result = serve_rows(jnp.concatenate([received, partner], 2), up_half, down_half)
    piece_slots = received.shape[2]
    from_partner = from_partner_2(result[:, :, piece_slots:], "expert", 0)
    summed = (
        result[:, :, :piece_slots].astype(jnp.float32) + from_partner.astype(jnp.float32)
    ).astype(jnp.bfloat16)
    returned = lax.all_to_all(summed, "expert", split_axis=0, concat_axis=0, tiled=True)
    flat_back = returned.reshape(-1, model_width)

    def back_index(slot_of, member):
        expert_id = slot_of // capacity
        within = slot_of % capacity
        return (
            (2 * expert_id + within // half_slots) * 2 + member
        ) * half_slots + within % half_slots

    index_fwd = back_index(slot_fwd, 0)
    index_bwd = back_index(slot_bwd, 1)
    layer_out = combine(x_fwd[0], flat_back[index_fwd], affinity_fwd[0])
    input_grad = combine(grad_bwd[0], flat_back[index_bwd], affinity_bwd[0])
    fwd_next = shifted(layer_out[None], "section", 1)
    bwd_next = shifted(input_grad[None], "section", -1)
    return (fwd_next, bwd_next)


def dense_weights(routes, affinity, experts):
    weights = affinity / jnp.sum(affinity, -1, keepdims=True)
    named = routes[:, :, None] == jnp.arange(experts, dtype=jnp.int32)
    return jnp.sum(jnp.where(named, weights[:, :, None], 0.0), 1)


def line_pairs(experts, low, high, by):
    return [
        (2 * z + half, 2 * (z + by) + half) for z in range(low, high) for half in range(2)
    ]


def after(value, *earlier):
    return lax.optimization_barrier((value, *earlier))[0]


def hop_out(blocks, step, experts):
    right = lax.ppermute(blocks[0], "expert", line_pairs(experts, step - 1, experts - 1, 1))
    left = lax.ppermute(blocks[1], "expert", line_pairs(experts, 1, experts - step + 1, -1))
    return (right, left)


def gather_lines(streams, experts):
    hops = [[(block, block)] for block in streams]
    order = []
    for step in range(1, experts):
        for stream in range(len(streams)):
            order.append((step + stream * 0.75, step, stream))
    order.sort()
    done = []
    for _, step, stream in order:
        blocks = hops[stream][step - 1]
        if len(done) >= 2:
            blocks = after(blocks, done[-2])
        landed = hop_out(blocks, step, experts)
        hops[stream].append(landed)
        done.append(landed)
    return hops


def line_rows(hops, experts, place):
    slots = [hops[0][0]]
    for ahead in range(1, experts):
        slots.append(
            jnp.where(place + ahead < experts, hops[ahead][1], hops[experts - ahead][0])
        )
    return jnp.concatenate(slots, 0)


def reduce_line(parts, experts):
    right, left = None, None
    for step in range(1, experts):
        send_right, send_left = parts[experts - step], parts[step]
        if right is not None:
            send_right = send_right + right.astype(jnp.float32)
            send_left = send_left + left.astype(jnp.float32)
        right = lax.ppermute(
            send_right.astype(jnp.bfloat16), "expert", line_pairs(experts, 0, step, 1)
        )
        left = lax.ppermute(
            send_left.astype(jnp.bfloat16),
            "expert",
            line_pairs(experts, experts - step, experts, -1),
        )
    return parts[0] + right.astype(jnp.float32) + left.astype(jnp.float32)


def own_expert_weights(dense, experts, place):
    columns = []
    for ahead in range(experts):
        target = lax.rem(place + experts - ahead, experts)
        column = lax.dynamic_index_in_dim(dense, target, 1, keepdims=False)
        if ahead:
            route = [
                (2 * z + half, 2 * ((z - ahead) % experts) + half)
                for z in range(experts)
                for half in range(2)
            ]
            column = lax.ppermute(column, "expert", route)
        columns.append(column)
    return jnp.concatenate(columns, 0)


AGAINST_ROWS = (((1,), (1,)), ((), ()))


def silu_rows(rows, up_part):
    return jax.nn.silu(jnp.dot(rows, up_part, preferred_element_type=jnp.float32)).astype(
        jnp.bfloat16
    )


def narrow_dot(rows, part):
    return jnp.dot(rows, part, preferred_element_type=jnp.float32).astype(jnp.bfloat16)


def narrow_dot_against(rows, part):
    return lax.dot_general(
        rows, part, AGAINST_ROWS, preferred_element_type=jnp.float32
    ).astype(jnp.bfloat16)


def pre_gradient(pre_act, rows_grad, down_parts):
    hidden_grad, low = 0.0, 0
    for part in down_parts:
        high = low + part.shape[1]
        hidden_grad += lax.dot_general(
            rows_grad[:, low:high], part, AGAINST_ROWS, preferred_element_type=jnp.float32
        )
        low = high
    return (hidden_grad * silu_grad(pre_act)).astype(jnp.bfloat16)


def weighted_blocks(first, second, weights, experts):
    total = (first.astype(jnp.float32) + second.astype(jnp.float32)) * weights[:, None]
    tokens = total.shape[0] // experts
    return [total[i * tokens : (i + 1) * tokens] for i in range(experts)]


def dense_path(
    x_fwd,
    routes_fwd,
    affinity_fwd,
    x_bwd,
    grad_bwd,
    routes_bwd,
    affinity_bwd,
    up_weight,
    down_weight,
):
    experts = lax.axis_size("expert") // 2
    place = lax.axis_index("expert") // 2
    up_half, down_half = up_weight[0], down_weight[0]
    width = x_fwd.shape[2]
    cuts = [(0, width // 2), (width // 2, width)]
    up_other = from_partner_2(up_half, "expert", 0)
    down_other = [
        from_partner_2(down_half[:, low:high], "expert", 0) for low, high in cuts
    ]
    hops_fwd, hops_saved, hops_grad = gather_lines([x_fwd[0], x_bwd[0], grad_bwd[0]], experts)
    weights_fwd = own_expert_weights(
        dense_weights(routes_fwd[0], affinity_fwd[0], experts), experts, place
    )
    weights_bwd = own_expert_weights(
        dense_weights(routes_bwd[0], affinity_bwd[0], experts), experts, place
    )
    rows_fwd = line_rows(hops_fwd, experts, place)
    hidden_own = silu_rows(rows_fwd, up_half)
    hidden_other = silu_rows(rows_fwd, up_other)
    fwd_next, last_parts = [], None
    for (low, high), down_part in zip(cuts, down_other):
        last_parts = weighted_blocks(
            narrow_dot(hidden_own, down_half[:, low:high]),
            narrow_dot(hidden_other, down_part),
            weights_fwd,
            experts,
        )
        summed = reduce_line(last_parts, experts)
        layer_out = (x_fwd[0][:, low:high].astype(jnp.float32) + summed).astype(jnp.bfloat16)
        fwd_next.append(shifted(layer_out, "section", 1))
    rows_saved = line_rows(hops_saved, experts, place)
    act_own = jnp.dot(rows_saved, up_half, preferred_element_type=jnp.float32)
    act_other = jnp.dot(rows_saved, up_other, preferred_element_type=jnp.float32)
    rows_grad = after(line_rows(hops_grad, experts, place), *last_parts)
    pre_own = pre_gradient(act_own, rows_grad, [down_half])
    pre_other = pre_gradient(act_other, rows_grad, down_other)
    bwd_next = []
    for low, high in cuts:
        parts = weighted_blocks(
            narrow_dot_against(pre_own, up_half[low:high]),
            narrow_dot_against(pre_other, up_other[low:high]),
            weights_bwd,
            experts,
        )
        summed = reduce_line(parts, experts)
        input_grad = (grad_bwd[0][:, low:high].astype(jnp.float32) + summed).astype(
            jnp.bfloat16
        )
        bwd_next.append(shifted(input_grad, "section", -1))
    return (jnp.concatenate(fwd_next, 1)[None], jnp.concatenate(bwd_next, 1)[None])


def per_device(*args):
    experts = lax.axis_size("expert") // 2
    top_count = args[1].shape[2]
    if 2 * top_count >= experts:
        return dense_path(*args)
    return general_path(*args)


def solution(mesh):
    in_specs = (
        P("section", "expert", None),
        P("section", "expert", None),
        P("section", "expert", None),
        P("section", "expert", None),
        P("section", "expert", None),
        P("section", "expert", None),
        P("section", "expert", None),
        P("section", None, "expert"),
        P("section", "expert", None),
    )
    out_specs = (P("section", "expert", None), P("section", "expert", None))
    return jax.shard_map(
        per_device, mesh=mesh, in_specs=in_specs, out_specs=out_specs, check_vma=False
    )
```

```python
import jax
import jax.numpy as jnp
from jax import lax
from jax.sharding import PartitionSpec as P


def from_partner_2(block, axis, apart):
    count = lax.axis_size(axis)
    route = []
    for low in range(count):
        high = low | 1 << apart
        if high != low and high < count:
            route += [(low, high), (high, low)]
    return lax.ppermute(block, axis, route)


def shifted(shard, axis, by):
    size = lax.axis_size(axis)
    return lax.ppermute(shard, axis, [(i, (i + by) % size) for i in range(size)])


def silu_grad(values):
    sigma = jax.nn.sigmoid(values)
    return sigma * (1.0 + values * (1.0 - sigma))


def slot_table(routes, experts, capacity):
    flat_routes = routes.reshape(-1)
    entries = flat_routes.shape[0]
    onehot = (flat_routes[:, None] == jnp.arange(experts, dtype=jnp.int32)[None, :]).astype(
        jnp.int32
    )
    before = jnp.cumsum(onehot, 0) - onehot
    position = jnp.sum(before * onehot, 1)
    slot_of = flat_routes * capacity + position
    source = (
        jnp.full((experts * capacity,), entries, jnp.int32)
        .at[slot_of]
        .set(jnp.arange(entries, dtype=jnp.int32))
    )
    return (slot_of, source)


def serve_rows(received, up_half, down_half):
    sources = received.shape[0]
    slots = received.shape[2]
    model_width = received.shape[3]
    row_count = sources * slots
    rows_fwd = received[:, 0].reshape(row_count, model_width)
    rows_saved = received[:, 1].reshape(row_count, model_width)
    rows_grad = received[:, 2].reshape(row_count, model_width)
    against_rows = (((1,), (1,)), ((), ()))
    hidden = jax.nn.silu(jnp.dot(rows_fwd, up_half, preferred_element_type=jnp.float32)).astype(
        jnp.bfloat16
    )
    part_fwd = jnp.dot(hidden, down_half, preferred_element_type=jnp.float32).astype(jnp.bfloat16)
    pre_act = jnp.dot(rows_saved, up_half, preferred_element_type=jnp.float32)
    hidden_grad = lax.dot_general(
        rows_grad, down_half, against_rows, preferred_element_type=jnp.float32
    )
    pre_grad = (hidden_grad * silu_grad(pre_act)).astype(jnp.bfloat16)
    part_bwd = lax.dot_general(
        pre_grad, up_half, against_rows, preferred_element_type=jnp.float32
    ).astype(jnp.bfloat16)
    return jnp.stack(
        [
            part_fwd.reshape(sources, slots, model_width),
            part_bwd.reshape(sources, slots, model_width),
        ],
        1,
    )


def combine(inputs, routed_rows, affinity):
    tokens = inputs.shape[0]
    top_count = affinity.shape[1]
    weights = affinity / jnp.sum(affinity, -1, keepdims=True)
    routed = routed_rows.reshape(tokens, top_count, inputs.shape[1]).astype(jnp.float32)
    return (inputs.astype(jnp.float32) + jnp.sum(weights[..., None] * routed, 1)).astype(
        jnp.bfloat16
    )


def general_path(
    x_fwd,
    routes_fwd,
    affinity_fwd,
    x_bwd,
    grad_bwd,
    routes_bwd,
    affinity_bwd,
    up_weight,
    down_weight,
):
    devices = lax.axis_size("expert")
    experts = devices // 2
    tokens = x_fwd.shape[1]
    model_width = x_fwd.shape[2]
    top_count = routes_fwd.shape[2]
    capacity = 3 * tokens * top_count // devices
    half_slots = capacity // 2
    up_half = up_weight[0]
    down_half = down_weight[0]
    slot_fwd, source_fwd = slot_table(routes_fwd[0], experts, capacity)
    slot_bwd, source_bwd = slot_table(routes_bwd[0], experts, capacity)
    zero_row = jnp.zeros((1, model_width), jnp.bfloat16)
    row_table = jnp.concatenate([x_fwd[0], zero_row, x_bwd[0], zero_row, grad_bwd[0], zero_row], 0)
    stride = tokens + 1
    token_fwd = (source_fwd // top_count).reshape(experts, capacity)
    token_bwd = (source_bwd // top_count).reshape(experts, capacity)
    gather_index = jnp.stack([token_fwd, token_bwd + stride, token_bwd + 2 * stride], 1)
    send_index = (
        gather_index.reshape(experts, 3, 2, half_slots)
        .transpose(0, 2, 1, 3)
        .reshape(devices, 3, half_slots)
    )
    outgoing = row_table[send_index]
    received = lax.all_to_all(outgoing, "expert", split_axis=0, concat_axis=0, tiled=True)
    partner = from_partner_2(received, "expert", 0)
    result = serve_rows(jnp.concatenate([received, partner], 2), up_half, down_half)
    piece_slots = received.shape[2]
    from_partner = from_partner_2(result[:, :, piece_slots:], "expert", 0)
    summed = (
        result[:, :, :piece_slots].astype(jnp.float32) + from_partner.astype(jnp.float32)
    ).astype(jnp.bfloat16)
    returned = lax.all_to_all(summed, "expert", split_axis=0, concat_axis=0, tiled=True)
    flat_back = returned.reshape(-1, model_width)

    def back_index(slot_of, member):
        expert_id = slot_of // capacity
        within = slot_of % capacity
        return (
            (2 * expert_id + within // half_slots) * 2 + member
        ) * half_slots + within % half_slots

    index_fwd = back_index(slot_fwd, 0)
    index_bwd = back_index(slot_bwd, 1)
    layer_out = combine(x_fwd[0], flat_back[index_fwd], affinity_fwd[0])
    input_grad = combine(grad_bwd[0], flat_back[index_bwd], affinity_bwd[0])
    fwd_next = shifted(layer_out[None], "section", 1)
    bwd_next = shifted(input_grad[None], "section", -1)
    return (fwd_next, bwd_next)


def dense_weights(routes, affinity, experts):
    weights = affinity / jnp.sum(affinity, -1, keepdims=True)
    named = routes[:, :, None] == jnp.arange(experts, dtype=jnp.int32)
    return jnp.sum(jnp.where(named, weights[:, :, None], 0.0), 1)


def line_pairs(experts, low, high, by):
    return [
        (2 * z + half, 2 * (z + by) + half) for z in range(low, high) for half in range(2)
    ]


def after(value, *earlier):
    return lax.optimization_barrier((value, *earlier))[0]


def end_pairs(experts, outward):
    pairs = []
    for half in range(2):
        inner_high, high = 2 * (experts - 2) + half, 2 * (experts - 1) + half
        inner_low, low = 2 + half, half
        pairs += [(inner_high, high), (inner_low, low)]
    return pairs if outward else [(target, source) for source, target in pairs]


def pass_on(block, pairs):
    return lax.ppermute(block, "expert", pairs) if pairs else None


def hop_out(blocks, step, experts, place, select):
    right = pass_on(blocks[0], line_pairs(experts, step - 1, experts - 2, 1))
    left = pass_on(blocks[1], line_pairs(experts, 2, experts - step + 1, -1))
    chosen = jnp.where(place == experts - 2, blocks[0], blocks[1])
    chosen = jnp.dot(select[step], chosen, preferred_element_type=jnp.float32)
    end = pass_on(chosen.astype(jnp.bfloat16), end_pairs(experts, True))
    return (right, left, end)


def gather_lines(streams, selects, experts, place):
    hops = [[(block, block)] for block in streams]
    order = []
    for step in range(1, experts):
        for stream in range(len(streams)):
            order.append((step + stream * 0.75, step, stream))
    order.sort()
    done = []
    for _, step, stream in order:
        blocks = hops[stream][step - 1][:2]
        if len(done) >= 2:
            blocks = after(blocks, done[-2])
        landed = hop_out(blocks, step, experts, place, selects[stream])
        hops[stream].append(landed)
        done.append([block for block in landed if block is not None])
    return hops


def line_rows(hops, experts, place):
    own = hops[0][0]
    at_end = (place == 0) | (place == experts - 1)
    slots = [own]
    for ahead in range(1, experts):
        end = hops[ahead][2]
        end = jnp.pad(end, ((0, own.shape[0] - end.shape[0]), (0, 0)))
        right, left = hops[experts - ahead][0], hops[ahead][1]
        if right is not None and left is not None:
            inner = jnp.where(place + ahead < experts, left, right)
        else:
            inner = left if right is None else right
        slots.append(jnp.where(at_end, end, inner))
    return jnp.concatenate(slots, 0)


def reduce_line(rows, weights, select, end_weights, experts, place):
    tokens = weights[0].shape[0]
    kept = select[1].shape[0]

    def part(slot):
        return rows[slot * tokens : (slot + 1) * tokens] * weights[slot][:, None]

    right, left = None, None
    for step in range(1, experts):
        slot = experts - step
        compact = rows[slot * tokens : slot * tokens + kept].astype(jnp.bfloat16)
        compact = pass_on(compact, end_pairs(experts, False))
        spread = lax.dot_general(
            select[slot], compact, (((0,), (0,)), ((), ())), preferred_element_type=jnp.float32
        )
        spread = spread * end_weights[slot][:, None]
        next_right = jnp.where(place == 1, spread, 0.0)
        next_left = jnp.where(place == experts - 2, spread, 0.0)
        if step > 1:
            send_right = (part(experts - step) + right).astype(jnp.bfloat16)
            send_left = (part(step) + left).astype(jnp.bfloat16)
            next_right += pass_on(send_right, line_pairs(experts, 1, step, 1)).astype(jnp.float32)
            next_left += pass_on(
                send_left, line_pairs(experts, experts - step, experts - 1, -1)
            ).astype(jnp.float32)
        right, left = next_right, next_left
    return part(0) + right + left


def column_weights(dense, experts):
    blocks = [dense]
    for ahead in range(1, experts):
        route = [
            (2 * z + half, 2 * ((z - ahead) % experts) + half)
            for z in range(experts)
            for half in range(2)
        ]
        blocks.append(lax.ppermute(dense, "expert", route))
    return blocks


def route_tables(blocks, experts, place, kept):
    own = [lax.dynamic_index_in_dim(block, place, 1, keepdims=False) for block in blocks]
    tokens = own[0].shape[0]
    earlier = jnp.triu(jnp.ones((tokens, tokens), jnp.bfloat16), 1)
    end_weights, select = [None], [None]
    for step in range(1, experts):
        high = blocks[(experts - step + 1) % experts][:, experts - 1]
        weight = jnp.where(place == experts - 2, high, blocks[step - 1][:, 0])
        named = weight != 0.0
        position = jnp.dot(
            named.astype(jnp.bfloat16)[None], earlier, preferred_element_type=jnp.float32
        )
        slot = jnp.arange(kept, dtype=jnp.int32)[:, None]
        select.append(
            ((position.astype(jnp.int32) == slot) & named[None]).astype(jnp.bfloat16)
        )
        end_weights.append(weight)
    return (own, select, end_weights)


AGAINST_ROWS = (((1,), (1,)), ((), ()))


def silu_rows(rows, up_part):
    return jax.nn.silu(jnp.dot(rows, up_part, preferred_element_type=jnp.float32)).astype(
        jnp.bfloat16
    )


def narrow_dot(rows, part):
    return jnp.dot(rows, part, preferred_element_type=jnp.float32).astype(jnp.bfloat16)


def narrow_dot_against(rows, part):
    return lax.dot_general(
        rows, part, AGAINST_ROWS, preferred_element_type=jnp.float32
    ).astype(jnp.bfloat16)


def pre_gradient(pre_act, rows_grad, down_parts):
    hidden_grad, low = 0.0, 0
    for part in down_parts:
        high = low + part.shape[1]
        hidden_grad += lax.dot_general(
            rows_grad[:, low:high], part, AGAINST_ROWS, preferred_element_type=jnp.float32
        )
        low = high
    return (hidden_grad * silu_grad(pre_act)).astype(jnp.bfloat16)


def both_halves(first, second):
    total = first.astype(jnp.float32) + second.astype(jnp.float32)
    return total.astype(jnp.bfloat16).astype(jnp.float32)


def dense_path(
    x_fwd,
    routes_fwd,
    affinity_fwd,
    x_bwd,
    grad_bwd,
    routes_bwd,
    affinity_bwd,
    up_weight,
    down_weight,
):
    experts = lax.axis_size("expert") // 2
    place = lax.axis_index("expert") // 2
    up_half, down_half = up_weight[0], down_weight[0]
    width = x_fwd.shape[2]
    cuts = [(0, width // 2), (width // 2, width)]
    up_other = from_partner_2(up_half, "expert", 0)
    down_other = [
        from_partner_2(down_half[:, low:high], "expert", 0) for low, high in cuts
    ]
    kept = 3 * x_fwd.shape[1] * routes_fwd.shape[2] // lax.axis_size("expert")
    tables = []
    for routes, affinity in ((routes_fwd, affinity_fwd), (routes_bwd, affinity_bwd)):
        dense = dense_weights(routes[0], affinity[0], experts)
        tables.append(route_tables(column_weights(dense, experts), experts, place, kept))
    (own_fwd, select_fwd, end_fwd), (own_bwd, select_bwd, end_bwd) = tables
    hops_fwd, hops_saved, hops_grad = gather_lines(
        [x_fwd[0], x_bwd[0], grad_bwd[0]], [select_fwd, select_bwd, select_bwd], experts, place
    )
    rows_fwd = line_rows(hops_fwd, experts, place)
    hidden_own = silu_rows(rows_fwd, up_half)
    hidden_other = silu_rows(rows_fwd, up_other)
    fwd_next, last_parts = [], None
    for (low, high), down_part in zip(cuts, down_other):
        last_parts = both_halves(
            narrow_dot(hidden_own, down_half[:, low:high]),
            narrow_dot(hidden_other, down_part),
        )
        summed = reduce_line(last_parts, own_fwd, select_fwd, end_fwd, experts, place)
        layer_out = (x_fwd[0][:, low:high].astype(jnp.float32) + summed).astype(jnp.bfloat16)
        fwd_next.append(shifted(layer_out, "section", 1))
    rows_saved = line_rows(hops_saved, experts, place)
    act_own = jnp.dot(rows_saved, up_half, preferred_element_type=jnp.float32)
    act_other = jnp.dot(rows_saved, up_other, preferred_element_type=jnp.float32)
    rows_grad = after(line_rows(hops_grad, experts, place), last_parts)
    pre_own = pre_gradient(act_own, rows_grad, [down_half])
    pre_other = pre_gradient(act_other, rows_grad, down_other)
    bwd_next = []
    for low, high in cuts:
        parts = both_halves(
            narrow_dot_against(pre_own, up_half[low:high]),
            narrow_dot_against(pre_other, up_other[low:high]),
        )
        summed = reduce_line(parts, own_bwd, select_bwd, end_bwd, experts, place)
        input_grad = (grad_bwd[0][:, low:high].astype(jnp.float32) + summed).astype(
            jnp.bfloat16
        )
        bwd_next.append(shifted(input_grad, "section", -1))
    return (jnp.concatenate(fwd_next, 1)[None], jnp.concatenate(bwd_next, 1)[None])


def per_device(*args):
    experts = lax.axis_size("expert") // 2
    top_count = args[1].shape[2]
    if 2 * top_count >= experts >= 4:
        return dense_path(*args)
    return general_path(*args)


def solution(mesh):
    in_specs = (
        P("section", "expert", None),
        P("section", "expert", None),
        P("section", "expert", None),
        P("section", "expert", None),
        P("section", "expert", None),
        P("section", "expert", None),
        P("section", "expert", None),
        P("section", None, "expert"),
        P("section", "expert", None),
    )
    out_specs = (P("section", "expert", None), P("section", "expert", None))
    return jax.shard_map(
        per_device, mesh=mesh, in_specs=in_specs, out_specs=out_specs, check_vma=False
    )
```
